32 devices in a mesh: tri: 32 (over z, y, x, core).
Axes of the slice: x: 2, y: 2, z: 4, core: 2. Of those that a mesh axis runs over, the one named last changes fastest.
Arguments:
- amplitudes: bfloat16 [32, 2816, 5632], P('tri'), as said below
- factors: bfloat16 [22528, 1280], P('tri'), may hold values from -2.5 to 2.5
- occ_energy: float32 [44], replicated, may hold values from -3 to -0.5
- virt_energy: float32 [512], replicated, may hold values from 0.2 to 6
Outputs:
- new_amplitudes: float32 [32, 2816, 5632], P('tri')
The draws below stay inside these ranges and needn't reach their ends.
Inputs may be any that keep to these rules, and one draw needn't show every extreme that they name: `amplitudes`: the matrix T assembled from the tiles is symmetric.
All inputs are finite; a program needn't handle non-finite values.
Results may differ from the reference program's by a relative error of at most 0.0069.
Values may be sent and summed in bfloat16 or wider, within the bound.
A program may use at most 192 MiB of HBM per device.

```python
import math
import jax
import jax.numpy as jnp
from jax import lax

OCC = 44
VIRT = 512
NAUX = 1280
STRIPES = 8
OV = 22528
ROWS = 704
BAND = 4
N_TRI = 32


def draw_amplitudes(key, part):
    scale = 0.7 / OV ** 0.5
    indices = jnp.arange(N_TRI, dtype=jnp.int32)

    def block_row(upper):

        def one_block(lower):
            small = jnp.minimum(upper, lower)
            large = jnp.maximum(upper, lower)
            subkey = jax.random.fold_in(key, small * N_TRI + large)
            values = jax.random.normal(subkey, (ROWS, ROWS), jnp.float32)
            values = jnp.where(upper == lower, (values + values.T) * 0.70710678, values)
            values = jnp.where(upper > lower, values.T, values)
            return (values * scale).astype(jnp.bfloat16)
        return jax.vmap(one_block)(indices)
    blocks = lax.map(block_row, indices)
    blocks = blocks.reshape(STRIPES, BAND, STRIPES, BAND, ROWS, ROWS)
    blocks = blocks.transpose(0, 3, 1, 4, 2, 5)
    return blocks.reshape(N_TRI, BAND * ROWS, STRIPES * ROWS)


def block_levels(rng, extent, cuts, least, high):
    loudness = 1.0
    for dim, parts in cuts:
        heights = jax.random.uniform(jax.random.fold_in(jax.random.fold_in(rng, 6), dim), (parts,), jnp.float32, least / len(cuts), high / len(cuts))
        loudness = loudness * jnp.repeat(jnp.exp(heights), extent[dim] // parts).reshape((-1,) + (1,) * (len(extent) - 1 - dim))
    return loudness


def centred(rng, dims, scale, bound, split=(), kind=jnp.bfloat16):
    level = block_levels(rng, dims, split, -0.22, 0.18) if split else 1.0
    array = jax.random.normal(rng, dims, jnp.float32) * scale * level
    return jnp.minimum(jnp.maximum(array, -bound), bound).astype(kind)


def setup_inputs(seed: int = 0) -> dict:
    arg_keys = jax.random.split(jax.random.key(seed), 5)
    return {
        "amplitudes": draw_amplitudes(jax.random.fold_in(arg_keys[4], 71), 0),
        "factors": centred(arg_keys[1], (OV, NAUX), 0.35, 2.5, ((0, 32),)),
        "occ_energy": jnp.clip(jax.random.uniform(arg_keys[2], (OCC,), jnp.float32, -3.0, -0.5), -3.0, -0.5),
        "virt_energy": jnp.clip(jnp.exp(jax.random.uniform(arg_keys[3], (VIRT,), jnp.float32, math.log(0.2), math.log(6.0))), 0.2, 6.0),
    }


def reference(amplitudes, factors, occ_energy, virt_energy):
    pair_energy = (virt_energy[None, :] - occ_energy[:, None]).reshape(OCC * VIRT)
    column_sets = factors.reshape(STRIPES, BAND, ROWS, NAUX).transpose(1, 0, 2, 3).reshape(BAND, STRIPES * ROWS, NAUX)
    tiles = amplitudes.reshape(STRIPES, BAND, BAND * ROWS, STRIPES * ROWS)

    def band_images(tile_row):
        def accumulate(total, pair):
            return total + jnp.dot(pair[0], pair[1], preferred_element_type=jnp.float32), None

        start = jnp.zeros((BAND * ROWS, NAUX), jnp.float32)
        total, unused = lax.scan(accumulate, start, (tile_row, column_sets))
        return total

    images = lax.map(band_images, tiles).reshape(OV, NAUX) + factors.astype(jnp.float32)
    dressed = images.astype(jnp.bfloat16)
    dressed_bands = dressed.reshape(STRIPES, BAND * ROWS, NAUX)
    dressed_sets = dressed.reshape(STRIPES, BAND, ROWS, NAUX).transpose(1, 0, 2, 3).reshape(BAND, STRIPES * ROWS, NAUX)
    energy_bands = pair_energy.reshape(STRIPES, BAND * ROWS)
    energy_sets = pair_energy.reshape(STRIPES, BAND, ROWS).transpose(1, 0, 2).reshape(BAND, STRIPES * ROWS)

    def one_tile(index):
        stripe = index // BAND
        column = index % BAND
        inner = jnp.dot(dressed_bands[stripe], dressed_sets[column].T, preferred_element_type=jnp.float32)
        return -inner / (energy_bands[stripe][:, None] + energy_sets[column][None, :])

    return lax.map(one_tile, jnp.arange(N_TRI, dtype=jnp.int32))
```

```python
import functools

import jax
import jax.numpy as jnp
from jax import lax
from jax.experimental import pallas as pl
from jax.experimental.pallas import tpu as pltpu
from jax.sharding import PartitionSpec as P


STRIPES = 8
SIDES = 2
PLACES = STRIPES // SIDES
VMEM = 60 * 2**20


def send(value, target):
    count = lax.axis_size("tri")
    return lax.ppermute(value, "tri", [(source, target(source)) for source in range(count)])


def set_gather(own, band_size):
    def along(step):
        def target(source):
            stripe, column = source // band_size, source % band_size
            place, side = stripe // SIDES, stripe % SIDES
            return ((place + step) % PLACES * SIDES + side) * band_size + column

        return target

    def across(source):
        return source // band_size * band_size ^ band_size | source % band_size

    near = [own] + [send(own, along(step)) for step in range(1, PLACES)]
    far = [send(piece, across) for piece in near]
    return near, far


def row_block(rows):
    block = rows
    while block > 352 and block % 32 == 0:
        block //= 2
    return block


def fill(held, pieces, place, side, rows, units):
    near, far = pieces
    for near_ref, far_ref, unit in zip(near, far, units):
        at = 0 if len(units) == 1 else lax.rem(place - unit + PLACES, PLACES) * SIDES
        for ref, part in ((near_ref, side), (far_ref, 1 - side)):
            held[pl.ds(pl.multiple_of((at + part) * rows, 16), rows), :] = ref[...]


def terms_kernel(rows, steps, where_ref, tile_ref, *refs):
    near, far = refs[:PLACES], refs[PLACES : 2 * PLACES]
    sent_ref, kept_ref, held = refs[2 * PLACES :]
    step = pl.program_id(0)

    @pl.when(step == 0)
    def _():
        fill(held, (near, far), where_ref[0], where_ref[1], rows, range(PLACES))

    product = jnp.dot(tile_ref[0], held[...], preferred_element_type=jnp.float32)
    product = product.astype(sent_ref.dtype)

    @pl.when(step < steps)
    def _():
        sent_ref[0] = product

    @pl.when(step >= steps)
    def _():
        kept_ref[0] = product


def image_terms(amplitudes, pieces, where, half, band_size):
    near, far = pieces
    rows, width = near[0].shape
    columns = amplitudes.shape[2]
    block = row_block(rows)
    parts = rows // block
    pairs = band_size // 4
    steps = pairs * parts

    def tile_index(step, where_ref):
        top, low = where_ref[2], where_ref[3]
        top = top if half else 1 - top
        second = step // steps
        place = step % steps // parts * 2 + jnp.where(second == 0, 1 - low, low)
        return 0, (top * pairs * 2 + place) * parts + step % parts, 0

    def sent_index(step, where_ref):
        at = jnp.minimum(step, steps - 1)
        return at // parts, at % parts, 0

    def kept_index(step, where_ref):
        at = jnp.maximum(step - steps, 0)
        return at // parts, at % parts, 0

    whole = pl.BlockSpec((rows, width), lambda step, where_ref: (0, 0))
    out = jax.ShapeDtypeStruct((pairs, rows, width), jnp.bfloat16)
    return pl.pallas_call(
        functools.partial(terms_kernel, rows, steps),
        out_shape=(out, out),
        grid_spec=pltpu.PrefetchScalarGridSpec(
            num_scalar_prefetch=1,
            grid=(2 * steps,),
            in_specs=[pl.BlockSpec((1, block, columns), tile_index)] + [whole] * (2 * PLACES),
            out_specs=(
                pl.BlockSpec((1, block, width), sent_index),
                pl.BlockSpec((1, block, width), kept_index),
            ),
            scratch_shapes=[pltpu.VMEM((columns, width), jnp.bfloat16)],
        ),
        compiler_params=pltpu.CompilerParams(vmem_limit_bytes=VMEM),
        cost_estimate=pl.CostEstimate(
            flops=4 * steps * block * columns * width,
            bytes_accessed=4 * steps * block * columns,
            transcendentals=0,
        ),
    )(where, amplitudes, *near, *far)


def half_reduce(sent, kept, device, levels):
    received = send(sent, lambda source: source ^ 1)
    buffer = kept.astype(jnp.float32) + received.astype(jnp.float32)
    for level in range(1, levels):
        pairs = buffer.reshape(-1, 2, *buffer.shape[1:])
        bit = device // 2**level % 2
        keeping = lax.dynamic_index_in_dim(pairs, bit, 1, keepdims=False)
        outgoing = lax.dynamic_index_in_dim(pairs, 1 - bit, 1, keepdims=False)
        received = send(outgoing.astype(jnp.bfloat16), lambda source: source ^ 2**level)
        buffer = keeping + received.astype(jnp.float32)
    return buffer[0]


def band_gather(own, device, levels):
    rows, width = own.shape
    buffer = own[None]
    for level in reversed(range(levels)):
        received = send(buffer, lambda source: source ^ 2**level)
        bit = device // 2**level % 2
        first = jnp.where(bit == 0, buffer, received)
        second = jnp.where(bit == 0, received, buffer)
        buffer = jnp.stack([first, second], 1).reshape(-1, rows, width)
    return buffer.reshape(-1, width)


def update_kernel(rows, units, parts, chained, where_ref, *refs):
    bands = refs[:parts]
    refs = refs[parts:]
    count = len(units)
    near = [refs[part * count : (part + 1) * count] for part in range(parts)]
    refs = refs[parts * count :]
    far = [refs[part * count : (part + 1) * count] for part in range(parts)]
    refs = refs[parts * count :]
    row_ref, column_ref = refs[:2]
    refs = refs[2 + chained :]
    out_ref, held = refs[0], refs[1:]

    @pl.when(pl.program_id(0) == 0)
    def _():
        for part in range(parts):
            fill(held[part], (near[part], far[part]), where_ref[0], where_ref[1], rows, units)

    inner = None
    for part in range(parts):
        product = lax.dot_general(
            bands[part][...],
            held[part][...],
            (((1,), (1,)), ((), ())),
            preferred_element_type=jnp.float32,
        )
        inner = product if inner is None else inner + product
    out_ref[0] = -inner / (row_ref[...] + column_ref[0])


def update(bands, near, far, row_energy, column_energy, where, units, earlier):
    parts = len(bands)
    rows = near[0][0].shape[0]
    height = bands[0].shape[0]
    columns = STRIPES * rows
    span = len(units) * SIDES * rows
    block = row_block(rows)
    widths = [band.shape[1] for band in bands]

    def at(where_ref):
        return lax.rem(where_ref[0] - units[0] + PLACES, PLACES) if len(units) == 1 else 0

    chained = int(earlier is not None)
    held = [near[part][unit] for part in range(parts) for unit in units]
    held += [far[part][unit] for part in range(parts) for unit in units]
    in_specs = [pl.BlockSpec((block, width), lambda step, where_ref: (step, 0)) for width in widths]
    in_specs += [pl.BlockSpec(piece.shape, lambda step, where_ref: (0, 0)) for piece in held]
    in_specs += [
        pl.BlockSpec((block, 1), lambda step, where_ref: (step, 0)),
        pl.BlockSpec((1, 1, span), lambda step, where_ref: (at(where_ref), 0, 0)),
    ]
    operands = [where, *bands, *held, row_energy[:, None], column_energy.reshape(-1, 1, span)]
    aliases = {}
    if chained:
        aliases = {len(operands): 0}
        in_specs.append(pl.BlockSpec(memory_space=pl.ANY))
        operands.append(earlier)
    return pl.pallas_call(
        functools.partial(update_kernel, rows, units, parts, chained),
        out_shape=jax.ShapeDtypeStruct((1, height, columns), jnp.float32),
        grid_spec=pltpu.PrefetchScalarGridSpec(
            num_scalar_prefetch=1,
            grid=(height // block,),
            in_specs=in_specs,
            out_specs=pl.BlockSpec((1, block, span), lambda step, where_ref: (0, step, at(where_ref))),
            scratch_shapes=[pltpu.VMEM((span, width), jnp.bfloat16) for width in widths],
        ),
        input_output_aliases=aliases,
        compiler_params=pltpu.CompilerParams(vmem_limit_bytes=VMEM),
        cost_estimate=pl.CostEstimate(
            flops=2 * height * span * sum(widths),
            bytes_accessed=4 * height * span,
            transcendentals=0,
        ),
    )(*operands)


def part_bounds(naux):
    first = -(-naux // 512) * 256
    return [(0, first), (first, naux)]


def per_device(amplitudes, factors, occ_energy, virt_energy):
    device = lax.axis_index("tri")
    band_size = lax.axis_size("tri") // STRIPES
    levels = band_size.bit_length() - 1
    rows, naux = factors.shape
    stripe, column = device // band_size, device % band_size
    pair_energy = (virt_energy[None, :] - occ_energy[:, None]).reshape(-1)
    grid = pair_energy.reshape(STRIPES, band_size, rows)
    row_energy = lax.dynamic_index_in_dim(grid, stripe, 0, keepdims=False).reshape(-1)
    column_energy = lax.dynamic_index_in_dim(grid, column, 1, keepdims=False).reshape(-1)
    where = jnp.stack(
        [stripe // SIDES, stripe % SIDES, column // (band_size // 2), column % 2]
    ).astype(jnp.int32)

    bounds = part_bounds(naux)
    bands, near, far = [], [], []
    for start, end in bounds:
        own = factors[:, start:end]
        pieces = set_gather(own, band_size)
        halves = []
        for half in range(2):
            sent, kept = image_terms(amplitudes, pieces, where, half, band_size)
            halves.append(half_reduce(sent, kept, device, levels - 1))
        received = send(halves[0].astype(jnp.bfloat16), lambda source: source ^ band_size // 2)
        images = halves[1] + received.astype(jnp.float32) + own.astype(jnp.float32)
        dressed = images.astype(jnp.bfloat16)
        near_part, far_part = set_gather(dressed, band_size)
        near.append(near_part)
        far.append(far_part)
        bands.append(band_gather(dressed, device, levels))

    if rows * SIDES % 128:
        groups = [list(range(PLACES))]
    else:
        groups = [[unit] for unit in range(PLACES)]
    result = None
    for group in groups:
        result = update(bands, near, far, row_energy, column_energy, where, group, result)
    return result


def solution(mesh):
    placed = (P("tri", None, None), P("tri", None), P(), P())
    return jax.shard_map(
        per_device, mesh=mesh, in_specs=placed, out_specs=P("tri", None, None), check_vma=False
    )
```

```python
import functools

import jax
import jax.numpy as jnp
from jax import lax
from jax.experimental import pallas as pl
from jax.experimental.pallas import tpu as pltpu
from jax.sharding import PartitionSpec as P


STRIPES = 8
SIDES = 2
PLACES = STRIPES // SIDES
TOP, LOW, TURN = STRIPES, STRIPES + 1, STRIPES + 2
VMEM = 60 * 2**20


def send(value, target):
    count = lax.axis_size("tri")
    pairs = [(source, target(source)) for source in range(count)]
    return lax.ppermute(value, "tri", [pair for pair in pairs if pair[1] is not None])


def position(stripe):
    place, side = stripe // SIDES, stripe % SIDES
    return place + side * (STRIPES - 1 - 2 * place)


def stripe_at(position):
    up = position < PLACES
    return up * (SIDES * position) + (1 - up) * (2 * STRIPES - 1 - SIDES * position)


def ring_gather(own, band_size, forward):
    def hop(step):
        def target(source):
            stripe, column = source // band_size, source % band_size
            return stripe_at((position(stripe) + step) % STRIPES) * band_size + column

        return target

    pieces = {0: own}
    for step, hops in ((1, STRIPES // 2 - 1 + forward), (-1, STRIPES // 2 - forward)):
        held = own
        for count in range(1, hops + 1):
            held = send(held, hop(step))
            pieces[-step * count % STRIPES] = held
    return [pieces[distance] for distance in range(STRIPES)]


def across_gather(own, band_size):
    def target(source):
        stripe, column = source // band_size, source % band_size
        if stripe // SIDES in (0, PLACES - 1):
            return None
        return (stripe ^ 1) * band_size + column

    return send(own, target)


def row_block(rows):
    block = rows
    while block > 352 and block % 32 == 0:
        block //= 2
    return block


def fill_all(held, chunks, spans, where_ref, rows, sems):
    copies = []
    for index, (pieces, (start, end)) in enumerate(zip(chunks, spans)):
        for distance, piece in enumerate(pieces):
            at = pl.multiple_of(where_ref[distance] * rows, 16)
            into = held.at[pl.ds(at, rows), pl.ds(start, end - start)]
            copy = pltpu.make_async_copy(piece, into, sems.at[index, distance])
            copy.start()
            copies.append(copy)
    for copy in copies:
        copy.wait()


def terms_kernel(rows, steps, spans, where_ref, tile_ref, *refs):
    chunks = [refs[index * STRIPES : (index + 1) * STRIPES] for index in range(len(spans))]
    sent_ref, kept_ref, held, sems = refs[len(spans) * STRIPES :]
    step = pl.program_id(0)

    @pl.when(step == 0)
    def _():
        fill_all(held, chunks, spans, where_ref, rows, sems)

    product = jnp.dot(tile_ref[0], held[...], preferred_element_type=jnp.float32)
    product = product.astype(sent_ref.dtype)

    @pl.when(step < steps)
    def _():
        sent_ref[0] = product

    @pl.when(step >= steps)
    def _():
        kept_ref[0] = product


def image_terms(amplitudes, chunks, where, half, band_size):
    rows = chunks[0][0].shape[0]
    spans = chunk_spans([pieces[0].shape[1] for pieces in chunks])
    width = spans[-1][1]
    columns = amplitudes.shape[2]
    block = row_block(rows)
    parts = rows // block
    pairs = band_size // 4
    steps = pairs * parts

    def tile_index(step, where_ref):
        top, low = where_ref[TOP], where_ref[LOW]
        top = top if half else 1 - top
        second = step // steps
        place = step % steps // parts * 2 + jnp.where(second == 0, 1 - low, low)
        return 0, (top * pairs * 2 + place) * parts + step % parts, 0

    def sent_index(step, where_ref):
        at = jnp.minimum(step, steps - 1)
        return at // parts, at % parts, 0

    def kept_index(step, where_ref):
        at = jnp.maximum(step - steps, 0)
        return at // parts, at % parts, 0

    pieces = [piece for chunk in chunks for piece in chunk]
    out = jax.ShapeDtypeStruct((pairs, rows, width), jnp.bfloat16)
    return pl.pallas_call(
        functools.partial(terms_kernel, rows, steps, spans),
        out_shape=(out, out),
        grid_spec=pltpu.PrefetchScalarGridSpec(
            num_scalar_prefetch=1,
            grid=(2 * steps,),
            in_specs=[pl.BlockSpec((1, block, columns), tile_index)]
            + [pl.BlockSpec(memory_space=pl.ANY)] * len(pieces),
            out_specs=(
                pl.BlockSpec((1, block, width), sent_index),
                pl.BlockSpec((1, block, width), kept_index),
            ),
            scratch_shapes=[
                pltpu.VMEM((columns, width), jnp.bfloat16),
                pltpu.SemaphoreType.DMA((len(chunks), STRIPES)),
            ],
        ),
        compiler_params=pltpu.CompilerParams(vmem_limit_bytes=VMEM),
        cost_estimate=pl.CostEstimate(
            flops=4 * steps * block * columns * width,
            bytes_accessed=4 * steps * block * columns,
            transcendentals=0,
        ),
    )(where, amplitudes, *pieces)


def half_reduce(sent, kept, device, levels):
    received = send(sent, lambda source: source ^ 1)
    buffer = kept.astype(jnp.float32) + received.astype(jnp.float32)
    for level in range(1, levels):
        pairs = buffer.reshape(-1, 2, *buffer.shape[1:])
        bit = device // 2**level % 2
        keeping = lax.dynamic_index_in_dim(pairs, bit, 1, keepdims=False)
        outgoing = lax.dynamic_index_in_dim(pairs, 1 - bit, 1, keepdims=False)
        received = send(outgoing.astype(jnp.bfloat16), lambda source: source ^ 2**level)
        buffer = keeping + received.astype(jnp.float32)
    return buffer[0]


def band_gather(own, levels):
    blocks = {0: own}
    for level in reversed(range(levels)):
        for bits in list(blocks):
            other = bits ^ 2**level
            blocks[other] = send(blocks[bits], lambda source: source ^ 2**level)
    return [blocks[bits] for bits in range(2**levels)]


def band_kernel(spans, column_ref, *refs):
    pieces, (band_ref, sems) = refs[:-2], refs[-2:]
    count = len(pieces) // len(spans)
    rows = pieces[0].shape[0]
    copies = []
    for index, (start, end) in enumerate(spans):
        for bits in range(count):
            at = pl.multiple_of((column_ref[0] ^ bits) * rows, 16)
            into = band_ref.at[pl.ds(at, rows), pl.ds(start, end - start)]
            copy = pltpu.make_async_copy(pieces[index * count + bits], into, sems.at[index, bits])
            copy.start()
            copies.append(copy)
    for copy in copies:
        copy.wait()


def join_band(blocks, column):
    spans = chunk_spans([part[0].shape[1] for part in blocks])
    count, rows = len(blocks[0]), blocks[0][0].shape[0]
    shape = (count * rows, spans[-1][1])
    pieces = [block for part in blocks for block in part]
    return pl.pallas_call(
        functools.partial(band_kernel, spans),
        out_shape=jax.ShapeDtypeStruct(shape, jnp.bfloat16),
        grid_spec=pltpu.PrefetchScalarGridSpec(
            num_scalar_prefetch=1,
            grid=(1,),
            in_specs=[pl.BlockSpec(memory_space=pl.ANY)] * len(pieces),
            out_specs=pl.BlockSpec(shape, lambda step, column_ref: (0, 0)),
            scratch_shapes=[pltpu.SemaphoreType.DMA((len(spans), count))],
        ),
        compiler_params=pltpu.CompilerParams(vmem_limit_bytes=VMEM),
        cost_estimate=pl.CostEstimate(
            flops=2**30, bytes_accessed=4 * shape[0] * shape[1], transcendentals=0
        ),
    )(column.astype(jnp.int32)[None], *pieces)


def update_kernel(rows, turn, spans, keys, chained, where_ref, band_ref, *refs):
    chunks = []
    for names in keys:
        chunks.append(refs[: len(names)])
        refs = refs[len(names) :]
    row_ref, column_ref = refs[:2]
    out_ref, held, sems = refs[2 + chained :]

    @pl.when(pl.program_id(0) == 0)
    def _():
        if turn is None:
            fill_all(held, chunks, spans, where_ref, rows, sems)
            return
        waits = []
        for index, (pieces, names, (start, end)) in enumerate(zip(chunks, keys, spans)):
            for side in range(SIDES):
                distance = where_ref[TURN + 3 * turn + 1 + side]
                into = held.at[pl.ds(side * rows, rows), pl.ds(start, end - start)]
                for piece, name in zip(pieces, names):
                    copy = pltpu.make_async_copy(piece, into, sems.at[index, side])
                    wanted = distance == name[0]
                    for other in name[1:]:
                        wanted = wanted | (distance == other)
                    pl.when(wanted)(copy.start)
                waits.append(copy)
        for copy in waits:
            copy.wait()

    inner = lax.dot_general(
        band_ref[...], held[...], (((1,), (1,)), ((), ())), preferred_element_type=jnp.float32
    )
    out_ref[0] = -inner / (row_ref[...] + column_ref[0])


def update(band, chunks, keys, row_energy, column_energy, where, turn, earlier):
    rows = chunks[0][0].shape[0]
    height, depth = band.shape
    columns = STRIPES * rows
    span = columns if turn is None else SIDES * rows
    block = rows
    spans = chunk_spans([pieces[0].shape[1] for pieces in chunks])

    def at(where_ref):
        return 0 if turn is None else where_ref[TURN + 3 * turn]

    chained = int(earlier is not None)
    held = [piece for pieces in chunks for piece in pieces]
    in_specs = [pl.BlockSpec((block, depth), lambda step, where_ref: (step, 0))]
    in_specs += [pl.BlockSpec(memory_space=pl.ANY)] * len(held)
    in_specs += [
        pl.BlockSpec((block, 1), lambda step, where_ref: (step, 0)),
        pl.BlockSpec((1, 1, span), lambda step, where_ref: (at(where_ref), 0, 0)),
    ]
    operands = [where, band, *held, row_energy, column_energy.reshape(-1, 1, span)]
    aliases = {}
    if chained:
        aliases = {len(operands): 0}
        in_specs.append(pl.BlockSpec(memory_space=pl.ANY))
        operands.append(earlier)
    return pl.pallas_call(
        functools.partial(update_kernel, rows, turn, spans, keys, chained),
        out_shape=jax.ShapeDtypeStruct((1, height, columns), jnp.float32),
        grid_spec=pltpu.PrefetchScalarGridSpec(
            num_scalar_prefetch=1,
            grid=(height // block,),
            in_specs=in_specs,
            out_specs=pl.BlockSpec((1, block, span), lambda step, where_ref: (0, step, at(where_ref))),
            scratch_shapes=[
                pltpu.VMEM((span, depth), jnp.bfloat16),
                pltpu.SemaphoreType.DMA((len(chunks), STRIPES)),
            ],
        ),
        input_output_aliases=aliases,
        compiler_params=pltpu.CompilerParams(vmem_limit_bytes=VMEM),
        cost_estimate=pl.CostEstimate(
            flops=2 * height * span * depth,
            bytes_accessed=4 * height * span,
            transcendentals=0,
        ),
    )(*operands)


def chunk_spans(widths):
    spans, start = [], 0
    for width in widths:
        spans.append((start, start + width))
        start += width
    return spans


def split(width):
    first = -(-width // 256) * 128
    return [(0, first), (first, width)]


def per_device(amplitudes, factors, occ_energy, virt_energy):
    device = lax.axis_index("tri")
    band_size = lax.axis_size("tri") // STRIPES
    levels = band_size.bit_length() - 1
    rows, naux = factors.shape
    stripe, column = device // band_size, device % band_size
    pair_energy = (virt_energy[None, :] - occ_energy[:, None]).reshape(-1)
    grid = pair_energy.reshape(STRIPES, band_size, rows)
    row_energy = lax.dynamic_index_in_dim(grid, stripe, 0, keepdims=False).reshape(-1)
    column_energy = lax.dynamic_index_in_dim(grid, column, 1, keepdims=False).reshape(-1)
    place = stripe // SIDES
    here = position(stripe)
    table = [stripe_at((here + distance) % STRIPES) for distance in range(STRIPES)]
    table += [column // (band_size // 2), column % 2]
    for turn in range(PLACES):
        unit = place ^ turn
        table.append(unit)
        table += [(position(unit * SIDES + side) - here) % STRIPES for side in range(SIDES)]
    where = jnp.stack([jnp.asarray(entry, jnp.int32) for entry in table])

    first = naux // 512 * 256
    bands, gathered, beside = [], [], []
    for part, own in enumerate((factors[:, :first], factors[:, first:])):
        cuts = split(own.shape[1])
        chunks = [
            ring_gather(own[:, start:end], band_size, index == part % 2)
            for index, (start, end) in enumerate(cuts)
        ]
        halves = []
        for half in range(2):
            sent, kept = image_terms(amplitudes, chunks, where, half, band_size)
            halves.append(half_reduce(sent, kept, device, levels - 1))
        received = send(halves[0].astype(jnp.bfloat16), lambda source: source ^ band_size // 2)
        images = halves[1] + received.astype(jnp.float32) + own.astype(jnp.float32)
        dressed = images.astype(jnp.bfloat16)
        for index, (start, end) in enumerate(cuts):
            chunk = dressed[:, start:end]
            gathered.append(ring_gather(chunk, band_size, index == part % 2))
            beside.append(across_gather(chunk, band_size))
        bands.append(band_gather(dressed, levels))
    band = join_band(bands, column)

    row_energy = row_energy[:, None]
    energies = (row_energy, column_energy, where)
    whole = tuple((distance,) for distance in range(STRIPES))
    if rows * SIDES % 128:
        return update(band, gathered, [whole] * len(gathered), *energies, None, None)
    result = None
    for turn in range(PLACES):
        chunks, keys = [], []
        for pieces, other in zip(gathered, beside):
            reach = [d for d in range(STRIPES) if min(d, STRIPES - d) <= turn + 1]
            chunk = [pieces[d] for d in reach]
            names = [(d,) for d in reach]
            if turn == 0:
                chunk.append(other)
                names.append((3, 5))
            chunks.append(chunk)
            keys.append(tuple(names))
        result = update(band, chunks, keys, *energies, turn, result)
    return result


def solution(mesh):
    placed = (P("tri", None, None), P("tri", None), P(), P())
    return jax.shard_map(
        per_device, mesh=mesh, in_specs=placed, out_specs=P("tri", None, None), check_vma=False
    )
```

```python
import functools

import jax
import jax.numpy as jnp
from jax import lax
from jax.experimental import pallas as pl
from jax.experimental.pallas import tpu as pltpu
from jax.sharding import PartitionSpec as P


STRIPES = 8
SIDES = 2
PLACES = STRIPES // SIDES
PARTS = 2
TOP, LOW, TURN = STRIPES, STRIPES + 1, STRIPES + 2
VMEM = 60 * 2**20


def send(value, target):
    count = lax.axis_size("tri")
    pairs = [(source, target(source)) for source in range(count)]
    return lax.ppermute(value, "tri", [pair for pair in pairs if pair[1] is not None])


def position(stripe):
    place, side = stripe // SIDES, stripe % SIDES
    return place + side * (STRIPES - 1 - 2 * place)


def stripe_at(position):
    up = position < PLACES
    return up * (SIDES * position) + (1 - up) * (2 * STRIPES - 1 - SIDES * position)


def ring_gather(own, band_size, forward):
    def hop(step):
        def target(source):
            stripe, column = source // band_size, source % band_size
            return stripe_at((position(stripe) + step) % STRIPES) * band_size + column

        return target

    pieces = {0: own}
    for step, hops in ((1, STRIPES // 2 - 1 + forward), (-1, STRIPES // 2 - forward)):
        held = own
        for count in range(1, hops + 1):
            held = send(held, hop(step))
            pieces[-step * count % STRIPES] = held
    return [pieces[distance] for distance in range(STRIPES)]


def across_gather(own, band_size):
    def target(source):
        stripe, column = source // band_size, source % band_size
        if stripe // SIDES in (0, PLACES - 1):
            return None
        return (stripe ^ 1) * band_size + column

    return send(own, target)


def row_block(rows):
    block = rows
    while block > 352 and block % 32 == 0:
        block //= 2
    return block


def fill_all(held, chunks, spans, where_ref, rows, sems):
    copies = []
    for index, (pieces, (start, end)) in enumerate(zip(chunks, spans)):
        for distance, piece in enumerate(pieces):
            at = pl.multiple_of(where_ref[distance] * rows, 16)
            into = held.at[pl.ds(at, rows), pl.ds(start, end - start)]
            copy = pltpu.make_async_copy(piece, into, sems.at[index, distance])
            copy.start()
            copies.append(copy)
    for copy in copies:
        copy.wait()


def terms_kernel(rows, steps, spans, where_ref, tile_ref, *refs):
    chunks = [refs[index * STRIPES : (index + 1) * STRIPES] for index in range(len(spans))]
    sent_ref, kept_ref, held, sems = refs[len(spans) * STRIPES :]
    step = pl.program_id(0)

    @pl.when(step == 0)
    def _():
        fill_all(held, chunks, spans, where_ref, rows, sems)

    product = jnp.dot(tile_ref[0], held[...], preferred_element_type=jnp.float32)
    product = product.astype(sent_ref.dtype)

    @pl.when(step < steps)
    def _():
        sent_ref[0] = product

    @pl.when(step >= steps)
    def _():
        kept_ref[0] = product


def image_terms(amplitudes, chunks, where, half, band_size):
    rows = chunks[0][0].shape[0]
    spans = chunk_spans([pieces[0].shape[1] for pieces in chunks])
    width = spans[-1][1]
    columns = amplitudes.shape[2]
    block = row_block(rows)
    parts = rows // block
    pairs = band_size // 4
    steps = pairs * parts

    def tile_index(step, where_ref):
        top, low = where_ref[TOP], where_ref[LOW]
        top = top if half else 1 - top
        second = step // steps
        place = step % steps // parts * 2 + jnp.where(second == 0, 1 - low, low)
        return 0, (top * pairs * 2 + place) * parts + step % parts, 0

    def sent_index(step, where_ref):
        at = jnp.minimum(step, steps - 1)
        return at // parts, at % parts, 0

    def kept_index(step, where_ref):
        at = jnp.maximum(step - steps, 0)
        return at // parts, at % parts, 0

    pieces = [piece for chunk in chunks for piece in chunk]
    out = jax.ShapeDtypeStruct((pairs, rows, width), jnp.bfloat16)
    return pl.pallas_call(
        functools.partial(terms_kernel, rows, steps, spans),
        out_shape=(out, out),
        grid_spec=pltpu.PrefetchScalarGridSpec(
            num_scalar_prefetch=1,
            grid=(2 * steps,),
            in_specs=[pl.BlockSpec((1, block, columns), tile_index)]
            + [pl.BlockSpec(memory_space=pl.ANY)] * len(pieces),
            out_specs=(
                pl.BlockSpec((1, block, width), sent_index),
                pl.BlockSpec((1, block, width), kept_index),
            ),
            scratch_shapes=[
                pltpu.VMEM((columns, width), jnp.bfloat16),
                pltpu.SemaphoreType.DMA((len(chunks), STRIPES)),
            ],
        ),
        compiler_params=pltpu.CompilerParams(vmem_limit_bytes=VMEM),
        cost_estimate=pl.CostEstimate(
            flops=4 * steps * block * columns * width,
            bytes_accessed=4 * steps * block * columns,
            transcendentals=0,
        ),
    )(where, amplitudes, *pieces)


def half_reduce(sent, kept, device, levels):
    received = send(sent, lambda source: source ^ 1)
    buffer = kept.astype(jnp.float32) + received.astype(jnp.float32)
    for level in range(1, levels):
        pairs = buffer.reshape(-1, 2, *buffer.shape[1:])
        bit = device // 2**level % 2
        keeping = lax.dynamic_index_in_dim(pairs, bit, 1, keepdims=False)
        outgoing = lax.dynamic_index_in_dim(pairs, 1 - bit, 1, keepdims=False)
        received = send(outgoing.astype(jnp.bfloat16), lambda source: source ^ 2**level)
        buffer = keeping + received.astype(jnp.float32)
    return buffer[0]


def band_gather(own, levels):
    blocks = {0: own}
    for level in reversed(range(levels)):
        for bits in list(blocks):
            other = bits ^ 2**level
            blocks[other] = send(blocks[bits], lambda source: source ^ 2**level)
    return [blocks[bits] for bits in range(2**levels)]


def band_kernel(spans, column_ref, *refs):
    pieces, (band_ref, sems) = refs[:-2], refs[-2:]
    count = len(pieces) // len(spans)
    rows = pieces[0].shape[0]
    copies = []
    for index, (start, end) in enumerate(spans):
        for bits in range(count):
            at = pl.multiple_of((column_ref[0] ^ bits) * rows, 16)
            into = band_ref.at[pl.ds(at, rows), pl.ds(start, end - start)]
            copy = pltpu.make_async_copy(pieces[index * count + bits], into, sems.at[index, bits])
            copy.start()
            copies.append(copy)
    for copy in copies:
        copy.wait()


def join_band(blocks, column):
    spans = chunk_spans([part[0].shape[1] for part in blocks])
    count, rows = len(blocks[0]), blocks[0][0].shape[0]
    shape = (count * rows, spans[-1][1])
    pieces = [block for part in blocks for block in part]
    return pl.pallas_call(
        functools.partial(band_kernel, spans),
        out_shape=jax.ShapeDtypeStruct(shape, jnp.bfloat16),
        grid_spec=pltpu.PrefetchScalarGridSpec(
            num_scalar_prefetch=1,
            grid=(1,),
            in_specs=[pl.BlockSpec(memory_space=pl.ANY)] * len(pieces),
            out_specs=pl.BlockSpec(shape, lambda step, column_ref: (0, 0)),
            scratch_shapes=[pltpu.SemaphoreType.DMA((len(spans), count))],
        ),
        compiler_params=pltpu.CompilerParams(vmem_limit_bytes=VMEM),
        cost_estimate=pl.CostEstimate(
            flops=2**30, bytes_accessed=4 * shape[0] * shape[1], transcendentals=0
        ),
    )(column.astype(jnp.int32)[None], *pieces)


def update_kernel(rows, turn, spans, keys, chained, where_ref, band_ref, *refs):
    chunks = []
    for names in keys:
        chunks.append(refs[: len(names)])
        refs = refs[len(names) :]
    row_ref, column_ref = refs[:2]
    out_ref, held, sems = refs[2 + chained :]

    @pl.when(pl.program_id(0) == 0)
    def _():
        if turn is None:
            fill_all(held, chunks, spans, where_ref, rows, sems)
            return
        waits = []
        for index, (pieces, names, (start, end)) in enumerate(zip(chunks, keys, spans)):
            for side in range(SIDES):
                distance = where_ref[TURN + 3 * turn + 1 + side]
                into = held.at[pl.ds(side * rows, rows), pl.ds(start, end - start)]
                for piece, name in zip(pieces, names):
                    copy = pltpu.make_async_copy(piece, into, sems.at[index, side])
                    wanted = distance == name[0]
                    for other in name[1:]:
                        wanted = wanted | (distance == other)
                    pl.when(wanted)(copy.start)
                waits.append(copy)
        for copy in waits:
            copy.wait()

    inner = lax.dot_general(
        band_ref[...], held[...], (((1,), (1,)), ((), ())), preferred_element_type=jnp.float32
    )
    out_ref[0] = -inner / (row_ref[...] + column_ref[0])


def update(band, chunks, keys, row_energy, column_energy, where, turn, earlier):
    rows = chunks[0][0].shape[0]
    height, depth = band.shape
    columns = STRIPES * rows
    span = columns if turn is None else SIDES * rows
    block = rows
    spans = chunk_spans([pieces[0].shape[1] for pieces in chunks])

    def at(where_ref):
        return 0 if turn is None else where_ref[TURN + 3 * turn]

    chained = int(earlier is not None)
    held = [piece for pieces in chunks for piece in pieces]
    in_specs = [pl.BlockSpec((block, depth), lambda step, where_ref: (step, 0))]
    in_specs += [pl.BlockSpec(memory_space=pl.ANY)] * len(held)
    in_specs += [
        pl.BlockSpec((block, 1), lambda step, where_ref: (step, 0)),
        pl.BlockSpec((1, 1, span), lambda step, where_ref: (at(where_ref), 0, 0)),
    ]
    operands = [where, band, *held, row_energy, column_energy.reshape(-1, 1, span)]
    aliases = {}
    if chained:
        aliases = {len(operands): 0}
        in_specs.append(pl.BlockSpec(memory_space=pl.ANY))
        operands.append(earlier)
    return pl.pallas_call(
        functools.partial(update_kernel, rows, turn, spans, keys, chained),
        out_shape=jax.ShapeDtypeStruct((1, height, columns), jnp.float32),
        grid_spec=pltpu.PrefetchScalarGridSpec(
            num_scalar_prefetch=1,
            grid=(height // block,),
            in_specs=in_specs,
            out_specs=pl.BlockSpec((1, block, span), lambda step, where_ref: (0, step, at(where_ref))),
            scratch_shapes=[
                pltpu.VMEM((span, depth), jnp.bfloat16),
                pltpu.SemaphoreType.DMA((len(chunks), STRIPES)),
            ],
        ),
        input_output_aliases=aliases,
        compiler_params=pltpu.CompilerParams(vmem_limit_bytes=VMEM),
        cost_estimate=pl.CostEstimate(
            flops=2 * height * span * depth,
            bytes_accessed=4 * height * span,
            transcendentals=0,
        ),
    )(*operands)


def chunk_spans(widths):
    spans, start = [], 0
    for width in widths:
        spans.append((start, start + width))
        start += width
    return spans


def split(width):
    first = -(-width // 256) * 128
    return [(0, first), (first, width)]


def per_device(amplitudes, factors, occ_energy, virt_energy):
    device = lax.axis_index("tri")
    band_size = lax.axis_size("tri") // STRIPES
    levels = band_size.bit_length() - 1
    rows, naux = factors.shape
    stripe, column = device // band_size, device % band_size
    pair_energy = (virt_energy[None, :] - occ_energy[:, None]).reshape(-1)
    grid = pair_energy.reshape(STRIPES, band_size, rows)
    row_energy = lax.dynamic_index_in_dim(grid, stripe, 0, keepdims=False).reshape(-1)
    column_energy = lax.dynamic_index_in_dim(grid, column, 1, keepdims=False).reshape(-1)
    place = stripe // SIDES
    here = position(stripe)
    table = [stripe_at((here + distance) % STRIPES) for distance in range(STRIPES)]
    table += [column // (band_size // 2), column % 2]
    for turn in range(PLACES):
        unit = place ^ turn
        table.append(unit)
        table += [(position(unit * SIDES + side) - here) % STRIPES for side in range(SIDES)]
    where = jnp.stack([jnp.asarray(entry, jnp.int32) for entry in table])

    first = naux // 512 * 256
    bands, gathered, beside = [], [], []
    for part, own in enumerate((factors[:, :first], factors[:, first:])):
        cuts = split(own.shape[1])
        chunks = [
            ring_gather(own[:, start:end], band_size, index == part % 2)
            for index, (start, end) in enumerate(cuts)
        ]
        halves = []
        for half in range(2):
            sent, kept = image_terms(amplitudes, chunks, where, half, band_size)
            halves.append(half_reduce(sent, kept, device, levels - 1))
        received = send(halves[0].astype(jnp.bfloat16), lambda source: source ^ band_size // 2)
        images = halves[1] + received.astype(jnp.float32) + own.astype(jnp.float32)
        dressed = images.astype(jnp.bfloat16)
        for index, (start, end) in enumerate(cuts):
            chunk = dressed[:, start:end]
            gathered.append(ring_gather(chunk, band_size, index == part % 2))
            last = part == PARTS - 1
            beside.append(across_gather(chunk, band_size) if last else None)
        bands.append(band_gather(dressed, levels))
    band = join_band(bands, column)

    row_energy = row_energy[:, None]
    energies = (row_energy, column_energy, where)
    whole = tuple((distance,) for distance in range(STRIPES))
    if rows * SIDES % 128:
        return update(band, gathered, [whole] * len(gathered), *energies, None, None)
    result = None
    for turn in range(PLACES):
        chunks, keys = [], []
        for pieces, other in zip(gathered, beside):
            steps = turn + 1 if other is not None else max(turn + 1, PLACES - 1)
            reach = [d for d in range(STRIPES) if min(d, STRIPES - d) <= steps]
            chunk = [pieces[d] for d in reach]
            names = [(d,) for d in reach]
            if turn == 0 and other is not None:
                chunk.append(other)
                names.append((3, 5))
            chunks.append(chunk)
            keys.append(tuple(names))
        result = update(band, chunks, keys, *energies, turn, result)
    return result


def solution(mesh):
    placed = (P("tri", None, None), P("tri", None), P(), P())
    return jax.shard_map(
        per_device, mesh=mesh, in_specs=placed, out_specs=P("tri", None, None), check_vma=False
    )
```
